32 devices in a mesh: seq: 8 (over z, y), head: 4 (over x, core).
Axes of the slice: x: 2, y: 2, z: 4, core: 2. Of those that a mesh axis runs over, the one named last changes fastest.
Arguments:
- residual: bfloat16 [4096, 3072], P('seq', 'head'), may hold values from -6 to 6
- q_self: bfloat16 [4096, 3072], P('seq', 'head'), may hold values from -6 to 6
- k_self: bfloat16 [4096, 3072], P('seq', 'head'), may hold values from -6 to 6
- v_self: bfloat16 [4096, 3072], P('seq', 'head'), may hold values from -6 to 6
- w_out: bfloat16 [3072, 3072], P('head'), may hold values from -0.109375 to 0.109375
- norm_gain: float32 [3072], replicated, may hold values from 0.5 to 1.5
- w_query: bfloat16 [3072, 3072], P('seq', 'head')
- w_cache: bfloat16 [3072, 2048], P('seq', 'head')
- block_doc: int32 [8], replicated, may hold values from 0 to 2, never falling along the last dimension, each value on 1 to 4 neighbouring positions
- tail_len: int32 [8], replicated, may hold values from 1 to 512
Outputs:
- hidden: bfloat16 [4096, 3072], P('seq', 'head')
- cross_context: bfloat16 [4096, 3072], P('seq', 'head')
The draws below stay inside these ranges and needn't reach their ends.
Inputs may be any that keep to these rules, and one draw needn't show every extreme that they name: block_doc never falls along the blocks; each document covers 1 to 4 consecutive blocks, and some document covers exactly 4. `tail_len`: read only for the last block of a document.
All inputs are finite; a program needn't handle non-finite values.
Results may differ from the reference program's by a relative error of at most 0.0078.
Values may be sent and summed in bfloat16 or wider, within the bound.
A program may use at most 128 MiB of HBM per device.

```python
import math
import jax
import jax.numpy as jnp
import numpy as np
from jax import lax

D = 3072
HEADS = 24
KV_HEADS = 8
HEAD_DIM = 128
TOK_DEV = 512
WINDOW = 2048
DOC_MAX = 2560
WIN_BLOCKS = 4
DOC_BLOCKS = 5
NBLK = 8
TOKENS = 4096
SPAN_MAX = 4
DOC_COUNT = 3
N_HEAD = 4


def sign_vector(key, length):
    return jnp.where(jax.random.randint(key, (length,), 0, 2) == 0, -1.0, 1.0).astype(jnp.float32)


def picked_rows(key):
    every = max(2, TOK_DEV // 64)
    return jax.random.randint(key, (TOKENS,), 0, TOK_DEV) < every


def base_noise(key, shape):
    return jax.random.normal(jax.random.fold_in(key, 3), shape, jnp.float32)


def self_operand(key, member):
    width = HEADS * HEAD_DIM
    plan = jax.random.fold_in(key, 9001)
    picked = picked_rows(jax.random.fold_in(plan, 1))
    pattern = sign_vector(jax.random.fold_in(plan, 2), width)
    strength = jax.random.uniform(jax.random.fold_in(plan, 3), (TOKENS,), jnp.float32, 3.0, 5.5)
    spread = 0.4
    noise = base_noise(jax.random.fold_in(key, member), (TOKENS, width))
    aligned = strength[:, None] * pattern[None, :] + spread * noise
    mixed = jnp.where(picked[:, None], aligned, noise)
    return jnp.clip(mixed, -6.0, 6.0).astype(jnp.bfloat16)


def draw_q_self(key, part):
    return self_operand(key, 11)


def draw_k_self(key, part):
    return self_operand(key, 12)


def cross_patterns(key):
    plan = jax.random.fold_in(key, 9002)
    return (sign_vector(jax.random.fold_in(plan, 1), D), sign_vector(jax.random.fold_in(plan, 2), HEAD_DIM))


def draw_residual(key, part):
    feature_sign = cross_patterns(key)[0]
    plan = jax.random.fold_in(key, 9003)
    picked = picked_rows(jax.random.fold_in(plan, 1))
    strength = jax.random.uniform(jax.random.fold_in(plan, 2), (TOKENS,), jnp.float32, 2.0, 4.5)
    noise = base_noise(jax.random.fold_in(key, 13), (TOKENS, D))
    aligned = strength[:, None] * feature_sign[None, :] + 0.3 * noise
    mixed = jnp.where(picked[:, None], aligned, noise)
    return jnp.clip(mixed, -6.0, 6.0).astype(jnp.bfloat16)


def scaled_noise(key, columns):
    limit = 6.0 * D ** (-0.5)
    return jnp.clip(base_noise(key, (D, columns)) * D ** (-0.5), -limit, limit)


def draw_w_query(key, part):
    feature_sign, head_sign = cross_patterns(key)
    width = HEADS * HEAD_DIM
    noise = scaled_noise(jax.random.fold_in(key, 14), width)
    amounts = jax.random.uniform(jax.random.fold_in(key, 9005), (HEADS,), jnp.float32, 14.5, 24.5)
    columns = (amounts[:, None] * head_sign[None, :]).reshape(width)
    plant = feature_sign[:, None] * columns[None, :] / (D * HEAD_DIM ** 0.25)
    return (noise + plant).astype(jnp.bfloat16)


def draw_w_cache(key, part):
    feature_sign, head_sign = cross_patterns(key)
    group = KV_HEADS // N_HEAD
    width = 2 * KV_HEADS * HEAD_DIM
    noise = scaled_noise(jax.random.fold_in(key, 15), width)
    key_part = jnp.broadcast_to(16.0 * head_sign, (N_HEAD, group, HEAD_DIM))
    columns = jnp.stack([key_part, jnp.zeros_like(key_part)], axis=1).reshape(width)
    plant = feature_sign[:, None] * columns[None, :] / (D * HEAD_DIM ** 0.25)
    return (noise + plant).astype(jnp.bfloat16)


def with_ends(drawn, own_key, least, top_value):
    place = [jax.random.randint(jax.random.fold_in(own_key, axis), (), 0, length) for axis, length in enumerate(drawn.shape)]
    longest = drawn.shape.index(max(drawn.shape))
    next_to = place[:longest] + [(place[longest] + 1) % drawn.shape[longest]] + place[longest + 1:]
    return drawn.at[tuple(place)].set(least).at[tuple(next_to)].set(top_value)


def block_levels(own_key, shape, cuts, least, largest):
    factor_of = 1.0
    for axis_at, blocks in cuts:
        steps = jax.random.uniform(jax.random.fold_in(jax.random.fold_in(own_key, 6), axis_at), (blocks,), jnp.float32, least / len(cuts), largest / len(cuts))
        factor_of = factor_of * jnp.repeat(jnp.exp(steps), shape[axis_at] // blocks).reshape((-1,) + (1,) * (len(shape) - 1 - axis_at))
    return factor_of


def profile(count, total, most, lean):
    loads = [(1 << 20) // math.isqrt(standing ** lean) + 1 for standing in range(2, count + 1)]
    rest, holding = total - most - (count - 1), [1] * (count - 1)
    while rest > 0:
        free = [i for i in range(count - 1) if holding[i] < most]
        mass, remaining = sum([loads[i] for i in free]), rest
        for i in free:
            addition = min(most - holding[i], max(1, remaining * loads[i] // mass), rest)
            holding[i] = holding[i] + addition
            rest = rest - addition
    return np.array([most] + holding)


def uneven(own_key, amount, total, reach, lean):
    if amount == 2:
        one = jax.random.randint(own_key, (), max(1, total - reach), min(reach, total - 1) + 1)
        return jnp.stack([one, total - one])
    sizes = jnp.asarray(profile(amount, total, reach, lean), jnp.int32)
    pairs = (amount - 1) // 2
    giver, receiver = sizes[1:1 + 2 * pairs:2], sizes[2:2 + 2 * pairs:2]
    slack = jnp.minimum(giver - 1, reach - receiver)
    shifted = jax.random.randint(jax.random.fold_in(own_key, 1), (pairs,), 0, 1 << 20) % (slack + 1)
    sizes = sizes.at[1:1 + 2 * pairs:2].set(giver - shifted).at[2:2 + 2 * pairs:2].set(receiver + shifted)
    return sizes[jax.random.permutation(jax.random.fold_in(own_key, 2), amount)]


def bell_draw(stream_key, extent, scale, most, cuts=(), kind=jnp.bfloat16):
    entries = scale * jax.random.normal(stream_key, extent, jnp.float32)
    if cuts:
        entries = entries * block_levels(stream_key, extent, cuts, -0.22, 0.18)
    return jnp.clip(entries, -most, most).astype(kind)


def setup_inputs(seed: int = 0) -> dict:
    arg_keys = jax.random.split(jax.random.key(seed), 11)
    residual = draw_residual(jax.random.fold_in(arg_keys[10], 71), 0)
    q_self = draw_q_self(jax.random.fold_in(arg_keys[10], 71), 0)
    k_self = draw_k_self(jax.random.fold_in(arg_keys[10], 71), 0)
    v_self = bell_draw(arg_keys[3], (TOKENS, HEADS * HEAD_DIM), 1.0, 6.0, ((0, 8), (1, 4)))
    w_out = bell_draw(arg_keys[4], (HEADS * HEAD_DIM, D), (HEADS * HEAD_DIM) ** -0.5, 0.109375, ((0, 4),))
    norm_gain = jnp.clip(1.0 + 0.1 * jax.random.normal(arg_keys[5], (D,), jnp.float32), 0.5, 1.5)
    w_query = draw_w_query(jax.random.fold_in(arg_keys[10], 71), 0)
    w_cache = draw_w_cache(jax.random.fold_in(arg_keys[10], 71), 0)
    block_doc = jnp.searchsorted(jnp.cumsum(uneven(arg_keys[8], DOC_COUNT, NBLK, SPAN_MAX, 2)), jnp.arange(NBLK), side="right").astype(jnp.int32)
    tail_len = with_ends(jax.random.randint(arg_keys[9], (NBLK,), 1, TOK_DEV + 1), jax.random.fold_in(arg_keys[9], 1), 1, TOK_DEV).astype(jnp.int32)
    return dict(residual=residual, q_self=q_self, k_self=k_self, v_self=v_self, w_out=w_out, norm_gain=norm_gain, w_query=w_query, w_cache=w_cache, block_doc=block_doc, tail_len=tail_len)


EPSILON = 1e-06

def block_valid(block_doc, tail_len, tok_rows):
    following = jnp.concatenate([block_doc[1:], jnp.full((1,), -1, jnp.int32)])
    closing = following != block_doc
    within = jnp.arange(tok_rows, dtype=jnp.int32)
    return jnp.logical_or(jnp.logical_not(closing)[:, None], within[None, :] < tail_len[:, None])

def permitted(query_block, key_blocks, block_doc, valid_tokens, tok_rows, reach_tokens):
    inside = key_blocks >= 0
    safe_blocks = jnp.maximum(key_blocks, 0)
    own_doc = jnp.take(block_doc, query_block)
    same_doc = jnp.logical_and(inside, jnp.take(block_doc, safe_blocks) == own_doc)
    live_keys = jnp.logical_and(same_doc[:, None], jnp.take(valid_tokens, safe_blocks, axis=0))
    within = jnp.arange(tok_rows, dtype=jnp.int32)
    query_pos = query_block * tok_rows + within
    key_pos = (key_blocks[:, None] * tok_rows + within[None, :]).reshape(-1)
    distance = query_pos[:, None] - key_pos[None, :]
    near = jnp.logical_and(distance >= 0, distance < reach_tokens)
    return jnp.logical_and(near, live_keys.reshape(-1)[None, :])

def attend(queries, keys, values, allowed):
    row_count, head_count, head_dim = queries.shape
    group_size = head_count // keys.shape[1]
    scaling = 1.0 / math.sqrt(head_dim)

    def one_head(head_index):
        query_head = lax.dynamic_index_in_dim(queries, head_index, 1, keepdims=False)
        key_head = lax.dynamic_index_in_dim(keys, head_index // group_size, 1, keepdims=False)
        value_head = lax.dynamic_index_in_dim(values, head_index // group_size, 1, keepdims=False)
        scores = lax.dot_general(query_head, key_head, (((1,), (1,)), ((), ())), preferred_element_type=jnp.float32) * scaling
        scores = jnp.where(allowed, scores, -1e+30)
        row_peak = lax.optimization_barrier(jnp.max(scores, axis=1, keepdims=True))
        weights = jnp.exp(scores - row_peak)
        row_total = lax.optimization_barrier(jnp.sum(weights, axis=1, keepdims=True))
        blended = jnp.dot(weights.astype(jnp.bfloat16), value_head, preferred_element_type=jnp.float32)
        return (blended / row_total).astype(jnp.bfloat16)
    per_head = lax.map(one_head, jnp.arange(head_count, dtype=jnp.int32))
    return jnp.transpose(per_head, (1, 0, 2)).reshape(row_count, head_count * head_dim)

def reference(residual, q_self, k_self, v_self, w_out, norm_gain, w_query, w_cache, block_doc, tail_len):
    valid_tokens = block_valid(block_doc, tail_len, TOK_DEV)
    width_all = HEADS * HEAD_DIM
    win_rows = WIN_BLOCKS * TOK_DEV
    key_pad = jnp.concatenate([jnp.zeros((win_rows, width_all), jnp.bfloat16), k_self], axis=0)
    value_pad = jnp.concatenate([jnp.zeros((win_rows, width_all), jnp.bfloat16), v_self], axis=0)

    def self_block(block_index):
        row_start = block_index * TOK_DEV
        queries = lax.dynamic_slice_in_dim(q_self, row_start, TOK_DEV, 0).reshape(TOK_DEV, HEADS, HEAD_DIM)
        keys = lax.dynamic_slice_in_dim(key_pad, row_start, win_rows + TOK_DEV, 0).reshape(-1, HEADS, HEAD_DIM)
        values = lax.dynamic_slice_in_dim(value_pad, row_start, win_rows + TOK_DEV, 0).reshape(-1, HEADS, HEAD_DIM)
        key_blocks = block_index - WIN_BLOCKS + jnp.arange(WIN_BLOCKS + 1, dtype=jnp.int32)
        allowed = permitted(block_index, key_blocks, block_doc, valid_tokens, TOK_DEV, WINDOW)
        return attend(queries, keys, values, allowed)
    context = lax.map(self_block, jnp.arange(NBLK, dtype=jnp.int32)).reshape(TOKENS, width_all)
    projected = jnp.dot(context, w_out, preferred_element_type=jnp.float32)
    hidden = (residual.astype(jnp.float32) + projected).astype(jnp.bfloat16)
    wide = hidden.astype(jnp.float32)
    mean_square = lax.optimization_barrier(jnp.mean(wide * wide, axis=1, keepdims=True))
    normed = (wide * lax.rsqrt(mean_square + EPSILON) * norm_gain).astype(jnp.bfloat16)
    cross_queries = jnp.dot(normed, w_query, preferred_element_type=jnp.float32).astype(jnp.bfloat16)
    cache_rows = jnp.dot(normed, w_cache, preferred_element_type=jnp.float32).astype(jnp.bfloat16)
    cache_rows = cache_rows.reshape(TOKENS, N_HEAD, 2, KV_HEADS // N_HEAD, HEAD_DIM)
    cache_keys = cache_rows[:, :, 0].reshape(TOKENS, KV_HEADS * HEAD_DIM)
    cache_values = cache_rows[:, :, 1].reshape(TOKENS, KV_HEADS * HEAD_DIM)
    doc_rows = (DOC_BLOCKS - 1) * TOK_DEV
    cache_key_pad = jnp.concatenate([jnp.zeros((doc_rows, KV_HEADS * HEAD_DIM), jnp.bfloat16), cache_keys], axis=0)
    cache_value_pad = jnp.concatenate([jnp.zeros((doc_rows, KV_HEADS * HEAD_DIM), jnp.bfloat16), cache_values], axis=0)

    def cross_block(block_index):
        row_start = block_index * TOK_DEV
        queries = lax.dynamic_slice_in_dim(cross_queries, row_start, TOK_DEV, 0).reshape(TOK_DEV, HEADS, HEAD_DIM)
        keys = lax.dynamic_slice_in_dim(cache_key_pad, row_start, doc_rows + TOK_DEV, 0).reshape(-1, KV_HEADS, HEAD_DIM)
        values = lax.dynamic_slice_in_dim(cache_value_pad, row_start, doc_rows + TOK_DEV, 0).reshape(-1, KV_HEADS, HEAD_DIM)
        key_blocks = block_index - DOC_BLOCKS + 1 + jnp.arange(DOC_BLOCKS, dtype=jnp.int32)
        allowed = permitted(block_index, key_blocks, block_doc, valid_tokens, TOK_DEV, DOC_MAX)
        return attend(queries, keys, values, allowed)
    cross_context = lax.map(cross_block, jnp.arange(NBLK, dtype=jnp.int32)).reshape(TOKENS, width_all)
    return (hidden, cross_context)
```

```python
import functools
import math

import jax
import jax.numpy as jnp
from jax import lax
from jax.experimental import pallas as pl
from jax.experimental.pallas import tpu as pltpu
from jax.sharding import PartitionSpec as P

D = 3072
HEAD_DIM = 128
WINDOW = 2048
DOC_BLOCKS = 5
EPSILON = 1e-06
ROW_TILE = 256


def passed_along(block, axis, distance):
    devices = range(lax.axis_size(axis))
    route = [(i - distance, i) for i in devices if i - distance in devices]
    return lax.ppermute(block, axis, route)


def swapped(block, axis, flip):
    return lax.ppermute(block, axis, [(i, i ^ flip) for i in range(lax.axis_size(axis))])


def stage_kernel(offsets, window, first, last, facts, q_ref, *refs):
    pairs = [(refs[2 * i], refs[2 * i + 1]) for i in range(len(offsets))]
    rest = refs[2 * len(offsets):]
    if not first:
        acc_in, peak_in, total_in = rest[:3]
        rest = rest[3:]
    if last:
        out_ref = rest[0]
        acc, peak, total = rest[1:]
    else:
        acc, peak, total = rest
    rows = q_ref.shape[0]
    tile = min(ROW_TILE, rows)
    scaling = 1.0 / math.sqrt(HEAD_DIM)

    def scores_of(r, k):
        return (
            lax.dot_general(
                q_ref[pl.ds(r, tile), :], k, (((1,), (1,)), ((), ())),
                preferred_element_type=jnp.float32,
            )
            * scaling
        )

    if not first:
        acc[...] = acc_in[...]
        peak[...] = peak_in[...]
        total[...] = total_in[...]

    for (k_ref, v_ref), offset, slot in zip(pairs, offsets, range(len(offsets))):

        def one(offset=offset, k_ref=k_ref, v_ref=v_ref):
            for r in range(0, rows, tile):
                here = pl.ds(r, tile)
                keys = r + tile if offset == 0 else rows
                s = scores_of(r, k_ref[pl.ds(0, keys), :])
                if offset == 0:
                    q_at = r + lax.broadcasted_iota(jnp.int32, s.shape, 0)
                    k_at = lax.broadcasted_iota(jnp.int32, s.shape, 1)
                    s = jnp.where((k_at <= q_at) & (k_at < facts[0]), s, -1e30)
                elif offset * rows + rows - 1 >= window:
                    q_at = r + lax.broadcasted_iota(jnp.int32, s.shape, 0)
                    k_at = lax.broadcasted_iota(jnp.int32, s.shape, 1)
                    s = jnp.where(offset * rows + q_at - k_at < window, s, -1e30)
                top = jnp.max(s, axis=1, keepdims=True)
                if offset == 0:
                    w = jnp.exp(s - top)
                    part = jnp.dot(
                        w.astype(jnp.bfloat16), v_ref[pl.ds(0, keys), :],
                        preferred_element_type=jnp.float32,
                    )
                    acc[here, :] = part
                    total[here, :] = jnp.broadcast_to(
                        jnp.sum(w, axis=1, keepdims=True), (tile, HEAD_DIM)
                    )
                    peak[here, :] = jnp.broadcast_to(top, (tile, HEAD_DIM))
                else:
                    old = peak[here, :]
                    new = jnp.maximum(old, top)
                    w = jnp.exp(s - new[:, :1])
                    fade = jnp.exp(old - new)
                    part = jnp.dot(
                        w.astype(jnp.bfloat16), v_ref[...], preferred_element_type=jnp.float32
                    )
                    acc[here, :] = acc[here, :] * fade + part
                    total[here, :] = total[here, :] * fade + jnp.sum(w, axis=1, keepdims=True)
                    peak[here, :] = new

        if offset == 0:
            one()
        else:
            pl.when(facts[1 + offset] > 0)(one)

    if last:
        out_ref[...] = (acc[...] / total[...]).astype(jnp.bfloat16)


def attend_stage(facts, queries, blocks, offsets, kv_heads, state, window, last):
    rows, width = queries.shape
    heads = width // HEAD_DIM
    group = heads // kv_heads
    tall = pl.BlockSpec((rows, HEAD_DIM), lambda h, f: (0, h))
    key_spec = pl.BlockSpec((rows, HEAD_DIM), lambda h, f: (0, h // group))
    value_spec = pl.BlockSpec((rows, HEAD_DIM), lambda h, f: (0, kv_heads + h // group))
    operands, specs = [queries], [tall]
    for block in blocks:
        operands += [block, block]
        specs += [key_spec, value_spec]
    if state is not None:
        operands += list(state)
        specs += [tall] * 3
    wide = jax.ShapeDtypeStruct((rows, width), jnp.float32)
    if last:
        out_shape = jax.ShapeDtypeStruct((rows, width), jnp.bfloat16)
        out_specs = tall
        scratch = [pltpu.VMEM((rows, HEAD_DIM), jnp.float32)] * 3
    else:
        out_shape, out_specs, scratch = (wide,) * 3, (tall,) * 3, []
    flops = 4 * rows * rows * width * len(offsets) * 3
    return pl.pallas_call(
        functools.partial(stage_kernel, offsets, window, state is None, last),
        out_shape=out_shape,
        grid_spec=pltpu.PrefetchScalarGridSpec(
            num_scalar_prefetch=1, grid=(heads,), in_specs=specs, out_specs=out_specs,
            scratch_shapes=scratch,
        ),
        compiler_params=pltpu.CompilerParams(
            dimension_semantics=("arbitrary",), vmem_limit_bytes=32 * 1024 * 1024
        ),
        cost_estimate=pl.CostEstimate(
            flops=flops, bytes_accessed=rows * width * 2 * (2 + 2 * len(offsets)),
            transcendentals=0,
        ),
    )(facts, *operands)


def shared_over_head(block):
    size = lax.axis_size("head")
    held = [block]
    step = size // 2
    got = {0: block}
    while step >= 1:
        for flip in sorted(got):
            got[flip ^ step] = None if got[flip] is None else swapped(got[flip], "head", step)
        step //= 2
    held = [got[flip] for flip in range(size)]
    return held


def gathered_rows(block, barrier_on):
    size = lax.axis_size("seq")
    if size > 16:
        return lax.all_gather(block, "seq", axis=0, tiled=True)
    me = lax.axis_index("seq")
    rows, width = block.shape
    block, _ = lax.optimization_barrier((block, barrier_on))
    whole = jnp.zeros((rows * size, width), block.dtype)
    ring = [(i, (i + 2) % size) for i in range(size)]
    moving = block
    for step in range(size // 2):
        owner = lax.rem(me - 2 * step + size, size)
        across = swapped(moving, "seq", 1)
        whole = lax.dynamic_update_slice_in_dim(whole, moving, owner * rows, 0)
        whole = lax.dynamic_update_slice_in_dim(whole, across, (owner ^ 1) * rows, 0)
        if step + 1 < size // 2:
            moving = lax.ppermute(moving, "seq", ring)
    return whole


def local(
    residual, q_self, k_self, v_self, w_out, norm_gain, w_query, w_cache, block_doc, tail_len
):
    rows, width = q_self.shape
    local_heads = width // HEAD_DIM
    local_kv = w_cache.shape[1] // (2 * HEAD_DIM)
    seq_size, head_size = lax.axis_size("seq"), lax.axis_size("head")
    span = min(DOC_BLOCKS, seq_size // 2)
    far = list(range(1, span))
    me, my_head = lax.axis_index("seq"), lax.axis_index("head")

    own_doc = block_doc[me]
    following = jnp.where(me == seq_size - 1, -1, block_doc[jnp.minimum(me + 1, seq_size - 1)])
    live = jnp.where(following != own_doc, jnp.minimum(tail_len[me], rows), rows)
    earlier = me - jnp.arange(span, dtype=jnp.int32)
    same = jnp.logical_and(earlier >= 0, block_doc[jnp.maximum(earlier, 0)] == own_doc)
    facts = jnp.concatenate([live[None].astype(jnp.int32), same.astype(jnp.int32)])

    stacked = jnp.concatenate([k_self, v_self], axis=1)
    seen = [passed_along(stacked, "seq", offset) for offset in far]

    own_columns = residual.shape[1]
    out_pieces = []
    for flip in range(head_size):
        piece = lax.dynamic_slice_in_dim(w_out, (my_head ^ flip) * own_columns, own_columns, 1)
        out_pieces.append(piece if flip == 0 else swapped(piece, "head", flip))

    state = attend_stage(facts, q_self, [stacked], [0], local_heads, None, WINDOW, False)
    if len(far) > 1:
        state = attend_stage(
            facts, q_self, seen[:-1], far[:-1], local_heads, state, WINDOW, False
        )
    weights = gathered_rows(jnp.concatenate([w_query, w_cache], axis=1), seen[1 % len(far)])
    context = attend_stage(facts, q_self, seen[-1:], far[-1:], local_heads, state, WINDOW, True)

    contexts = shared_over_head(context)
    projected = jnp.dot(contexts[0], out_pieces[0], preferred_element_type=jnp.float32)
    for flip in range(1, head_size):
        projected += jnp.dot(contexts[flip], out_pieces[flip], preferred_element_type=jnp.float32)
    hidden = (residual.astype(jnp.float32) + projected).astype(jnp.bfloat16)

    full = jnp.zeros((rows, own_columns * head_size), jnp.bfloat16)
    for flip, piece in enumerate(shared_over_head(hidden)):
        full = lax.dynamic_update_slice_in_dim(full, piece, (my_head ^ flip) * own_columns, 1)
    wide = full.astype(jnp.float32)
    mean_square = jnp.sum(wide * wide, axis=1, keepdims=True) / D
    normed = (wide * lax.rsqrt(mean_square + EPSILON) * norm_gain).astype(jnp.bfloat16)

    cache_rows = jnp.dot(
        normed, weights[:, width:], preferred_element_type=jnp.float32
    ).astype(jnp.bfloat16)
    history = [passed_along(cache_rows, "seq", offset) for offset in far]
    cross_queries = jnp.dot(
        normed, weights[:, :width], preferred_element_type=jnp.float32
    ).astype(jnp.bfloat16)
    reach = DOC_BLOCKS * rows
    state = attend_stage(facts, cross_queries, [cache_rows], [0], local_kv, None, reach, False)
    cross_context = attend_stage(facts, cross_queries, history, far, local_kv, state, reach, True)
    return (hidden, cross_context)


def solution(mesh):
    in_specs = (
        P("seq", "head"),
        P("seq", "head"),
        P("seq", "head"),
        P("seq", "head"),
        P("head", None),
        P(),
        P("seq", "head"),
        P("seq", "head"),
        P(),
        P(),
    )
    out_specs = (P("seq", "head"), P("seq", "head"))
    return jax.shard_map(local, mesh=mesh, in_specs=in_specs, out_specs=out_specs, check_vma=False)
```

```python
import functools
import math

import jax
import jax.numpy as jnp
from jax import lax
from jax.experimental import pallas as pl
from jax.experimental.pallas import tpu as pltpu
from jax.sharding import PartitionSpec as P

D = 3072
HEAD_DIM = 128
WINDOW = 2048
DOC_BLOCKS = 5
EPSILON = 1e-06
ROW_TILE = 256


def passed_along(block, axis, distance):
    devices = range(lax.axis_size(axis))
    route = [(i - distance, i) for i in devices if i - distance in devices]
    return lax.ppermute(block, axis, route)


def swapped(block, axis, flip):
    return lax.ppermute(block, axis, [(i, i ^ flip) for i in range(lax.axis_size(axis))])


def stage_kernel(offsets, window, first, last, facts, q_ref, *refs):
    pairs = [(refs[2 * i], refs[2 * i + 1]) for i in range(len(offsets))]
    rest = refs[2 * len(offsets):]
    if not first:
        acc_in, peak_in, total_in = rest[:3]
        rest = rest[3:]
    if last:
        out_ref = rest[0]
        acc, peak, total = rest[1:]
    else:
        acc, peak, total = rest
    rows = q_ref.shape[0]
    tile = min(ROW_TILE, rows)
    scaling = math.log2(math.e) / math.sqrt(HEAD_DIM)

    def scores_of(r, k):
        return lax.dot_general(
            q_ref[pl.ds(r, tile), :], k, (((1,), (1,)), ((), ())),
            preferred_element_type=jnp.float32,
        )

    if not first:
        acc[...] = acc_in[...]
        peak[...] = peak_in[...]
        total[...] = total_in[...]

    for (k_ref, v_ref), (flag, offset) in zip(pairs, offsets):

        def one(offset=offset, k_ref=k_ref, v_ref=v_ref):
            for r in range(0, rows, tile):
                here = pl.ds(r, tile)
                keys = r + tile if offset == 0 else rows
                s = scores_of(r, k_ref[pl.ds(0, keys), :])
                if offset == 0:
                    q_at = r + lax.broadcasted_iota(jnp.int32, s.shape, 0)
                    k_at = lax.broadcasted_iota(jnp.int32, s.shape, 1)
                    s = jnp.where((k_at <= q_at) & (k_at < facts[0]), s, -1e30)
                elif offset * rows + rows - 1 >= window:
                    q_at = r + lax.broadcasted_iota(jnp.int32, s.shape, 0)
                    k_at = lax.broadcasted_iota(jnp.int32, s.shape, 1)
                    s = jnp.where(offset * rows + q_at - k_at < window, s, -1e30)
                top = jnp.max(s, axis=1, keepdims=True)
                if offset == 0:
                    w = jnp.exp2((s - top) * scaling)
                    part = jnp.dot(
                        w.astype(jnp.bfloat16), v_ref[pl.ds(0, keys), :],
                        preferred_element_type=jnp.float32,
                    )
                    acc[here, :] = part
                    total[here, :] = jnp.broadcast_to(
                        jnp.sum(w, axis=1, keepdims=True), (tile, HEAD_DIM)
                    )
                    peak[here, :] = jnp.broadcast_to(top, (tile, HEAD_DIM))
                else:
                    old = peak[here, :]
                    new = jnp.maximum(old, top)
                    w = jnp.exp2((s - new[:, :1]) * scaling)
                    fade = jnp.exp2((old - new) * scaling)
                    part = jnp.dot(
                        w.astype(jnp.bfloat16), v_ref[...], preferred_element_type=jnp.float32
                    )
                    acc[here, :] = acc[here, :] * fade + part
                    total[here, :] = total[here, :] * fade + jnp.sum(w, axis=1, keepdims=True)
                    peak[here, :] = new

        if offset == 0:
            one()
        else:
            pl.when(facts[flag] > 0)(one)

    if last:
        out_ref[...] = (acc[...] / total[...]).astype(jnp.bfloat16)


def attend_stage(facts, queries, blocks, offsets, kv_heads, state, window, last):
    rows, width = queries.shape
    heads = width // HEAD_DIM
    group = heads // kv_heads
    tall = pl.BlockSpec((rows, HEAD_DIM), lambda h, f: (0, h))
    key_spec = pl.BlockSpec((rows, HEAD_DIM), lambda h, f: (0, h // group))
    value_spec = pl.BlockSpec((rows, HEAD_DIM), lambda h, f: (0, kv_heads + h // group))
    operands, specs = [queries], [tall]
    for block in blocks:
        operands += [block, block]
        specs += [key_spec, value_spec]
    if state is not None:
        operands += list(state)
        specs += [tall] * 3
    wide = jax.ShapeDtypeStruct((rows, width), jnp.float32)
    if last:
        out_shape = jax.ShapeDtypeStruct((rows, width), jnp.bfloat16)
        out_specs = tall
        scratch = [pltpu.VMEM((rows, HEAD_DIM), jnp.float32)] * 3
    else:
        out_shape, out_specs, scratch = (wide,) * 3, (tall,) * 3, []
    flops = 4 * rows * rows * width * len(offsets) * 3
    return pl.pallas_call(
        functools.partial(stage_kernel, offsets, window, state is None, last),
        out_shape=out_shape,
        grid_spec=pltpu.PrefetchScalarGridSpec(
            num_scalar_prefetch=1, grid=(heads,), in_specs=specs, out_specs=out_specs,
            scratch_shapes=scratch,
        ),
        compiler_params=pltpu.CompilerParams(
            dimension_semantics=("arbitrary",), vmem_limit_bytes=32 * 1024 * 1024
        ),
        cost_estimate=pl.CostEstimate(
            flops=flops, bytes_accessed=rows * width * 2 * (2 + 2 * len(offsets)),
            transcendentals=0,
        ),
    )(facts, *operands)


def shared_over_head(block):
    size = lax.axis_size("head")
    held = [block]
    step = size // 2
    got = {0: block}
    while step >= 1:
        for flip in sorted(got):
            got[flip ^ step] = None if got[flip] is None else swapped(got[flip], "head", step)
        step //= 2
    held = [got[flip] for flip in range(size)]
    return held


def sent(block, routes):
    return lax.ppermute(block, "seq", routes)


def row_gather(block):
    size = lax.axis_size("seq")
    me = lax.axis_index("seq")
    ring = [(i, (i + 2) % size) for i in range(size)]
    steps = []
    moving = block
    for step in range(size // 2):
        owner = lax.rem(me - 2 * step + size, size)
        across = swapped(moving, "seq", 1)
        onward = sent(moving, ring) if step + 1 < size // 2 else None
        moving, across, onward = yield moving, across, onward, owner
        moving = onward


def placed(whole, piece, owner):
    return lax.dynamic_update_slice_in_dim(whole, piece, owner * piece.shape[0], 0)


def waves(block, odd, beside):
    size = lax.axis_size("seq")
    first = sent(block, [(i, i + 1) for i in range(size - 1)])
    second_even = sent(block, [(i, i + 2) for i in range(0, size - 2, 2)])
    if beside is not None:
        first, beside = lax.optimization_barrier((first, beside))
    mixed = jnp.where(odd, block, first)
    second = sent(mixed, [(i, i + 2) for i in range(size - 2)])
    third_odd = sent(second_even, [(i, i + 1) for i in range(2, size, 2)])
    return first, [second_even, second, third_odd], beside


def local(
    residual, q_self, k_self, v_self, w_out, norm_gain, w_query, w_cache, block_doc, tail_len
):
    rows, width = q_self.shape
    local_heads = width // HEAD_DIM
    local_kv = w_cache.shape[1] // (2 * HEAD_DIM)
    seq_size, head_size = lax.axis_size("seq"), lax.axis_size("head")
    span = min(DOC_BLOCKS, seq_size // 2)
    far = list(range(1, span))
    me, my_head = lax.axis_index("seq"), lax.axis_index("head")

    own_doc = block_doc[me]
    following = jnp.where(me == seq_size - 1, -1, block_doc[jnp.minimum(me + 1, seq_size - 1)])
    live = jnp.where(following != own_doc, jnp.minimum(tail_len[me], rows), rows)
    odd = lax.rem(me, 2) == 1
    small = span == 4 and seq_size % 2 == 0

    def together(distance):
        other = me - distance
        return jnp.logical_and(other >= 0, block_doc[jnp.maximum(other, 0)] == own_doc)

    if small:
        flags = [
            together(1),
            jnp.logical_and(jnp.logical_not(odd), together(2)),
            jnp.where(odd, together(2), together(3)),
            jnp.logical_and(odd, together(3)),
        ]
        distances = [1, 2, 3, 3]
    else:
        flags = [together(distance) for distance in far]
        distances = far
    facts = jnp.stack([live.astype(jnp.int32)] + [flag.astype(jnp.int32) for flag in flags])
    slots = [(1 + i, distance) for i, distance in enumerate(distances)]

    stacked = jnp.concatenate([k_self, v_self], axis=1)
    weight_rows = jnp.concatenate([w_query, w_cache], axis=1)
    state = attend_stage(facts, q_self, [stacked], [(0, 0)], local_heads, None, WINDOW, False)
    if small:
        near, late, state = waves(stacked, odd, state)
    else:
        near, *late = [passed_along(stacked, "seq", offset) for offset in far]

    own_columns = residual.shape[1]
    out_pieces = []
    for flip in range(head_size):
        piece = lax.dynamic_slice_in_dim(w_out, (my_head ^ flip) * own_columns, own_columns, 1)
        out_pieces.append(piece if flip == 0 else swapped(piece, "head", flip))

    state = attend_stage(facts, q_self, [near], slots[:1], local_heads, state, WINDOW, False)
    if small:
        weight_rows, state = lax.optimization_barrier((weight_rows, state))
        weights = jnp.zeros((weight_rows.shape[0] * seq_size, weight_rows.shape[1]), jnp.bfloat16)
        gather = row_gather(weight_rows)
        moving, across, onward, owner = next(gather)
        late, across, onward = lax.optimization_barrier((late, across, onward))
        weights = placed(placed(weights, moving, owner), across, owner ^ 1)
        moving, across, onward, owner = gather.send((moving, across, onward))
    else:
        weights = lax.all_gather(weight_rows, "seq", axis=0, tiled=True)
    context = attend_stage(facts, q_self, late, slots[1:], local_heads, state, WINDOW, True)
    if small:
        context, across, onward = lax.optimization_barrier((context, across, onward))
        weights = placed(placed(weights, moving, owner), across, owner ^ 1)
        moving, across, onward, owner = gather.send((moving, across, onward))

    contexts = shared_over_head(context)
    projected = jnp.dot(contexts[0], out_pieces[0], preferred_element_type=jnp.float32)
    for flip in range(1, head_size):
        projected += jnp.dot(contexts[flip], out_pieces[flip], preferred_element_type=jnp.float32)
    hidden = (residual.astype(jnp.float32) + projected).astype(jnp.bfloat16)
    if small:
        hidden, across, onward = lax.optimization_barrier((hidden, across, onward))
        weights = placed(placed(weights, moving, owner), across, owner ^ 1)
        while onward is not None:
            moving, across, onward, owner = gather.send((moving, across, onward))
            weights = placed(placed(weights, moving, owner), across, owner ^ 1)

    full = jnp.zeros((rows, own_columns * head_size), jnp.bfloat16)
    for flip, piece in enumerate(shared_over_head(hidden)):
        full = lax.dynamic_update_slice_in_dim(full, piece, (my_head ^ flip) * own_columns, 1)
    wide = full.astype(jnp.float32)
    mean_square = jnp.sum(wide * wide, axis=1, keepdims=True) / D
    normed = (wide * lax.rsqrt(mean_square + EPSILON) * norm_gain).astype(jnp.bfloat16)

    cache_rows = jnp.dot(
        normed, weights[:, width:], preferred_element_type=jnp.float32
    ).astype(jnp.bfloat16)
    if small:
        near, late, _ = waves(cache_rows, odd, None)
    else:
        near, *late = [passed_along(cache_rows, "seq", offset) for offset in far]
    cross_queries = jnp.dot(
        normed, weights[:, :width], preferred_element_type=jnp.float32
    ).astype(jnp.bfloat16)
    reach = DOC_BLOCKS * rows
    state = attend_stage(
        facts, cross_queries, [cache_rows, near], [(0, 0)] + slots[:1], local_kv, None, reach, False
    )
    cross_context = attend_stage(
        facts, cross_queries, late, slots[1:], local_kv, state, reach, True
    )
    return (hidden, cross_context)


def solution(mesh):
    in_specs = (
        P("seq", "head"),
        P("seq", "head"),
        P("seq", "head"),
        P("seq", "head"),
        P("head", None),
        P(),
        P("seq", "head"),
        P("seq", "head"),
        P(),
        P(),
    )
    out_specs = (P("seq", "head"), P("seq", "head"))
    return jax.shard_map(local, mesh=mesh, in_specs=in_specs, out_specs=out_specs, check_vma=False)
```

```python
import functools
import math

import jax
import jax.numpy as jnp
from jax import lax
from jax.experimental import pallas as pl
from jax.experimental.pallas import tpu as pltpu
from jax.sharding import PartitionSpec as P

D = 3072
HEAD_DIM = 128
WINDOW = 2048
DOC_BLOCKS = 5
EPSILON = 1e-06
ROW_TILE = 256


def passed_along(block, axis, distance):
    devices = range(lax.axis_size(axis))
    route = [(i - distance, i) for i in devices if i - distance in devices]
    return lax.ppermute(block, axis, route)


def swapped(block, axis, flip):
    return lax.ppermute(block, axis, [(i, i ^ flip) for i in range(lax.axis_size(axis))])


def stage_kernel(offsets, window, first, last, facts, q_ref, *refs):
    pairs = [(refs[2 * i], refs[2 * i + 1]) for i in range(len(offsets))]
    rest = refs[2 * len(offsets):]
    if not first:
        acc_in, peak_in, total_in = rest[:3]
        rest = rest[3:]
    if last:
        out_ref = rest[0]
        acc, peak, total = rest[1:]
    else:
        acc, peak, total = rest
    rows = q_ref.shape[0]
    tile = min(ROW_TILE, rows)
    scaling = math.log2(math.e) / math.sqrt(HEAD_DIM)

    def scores_of(r, k):
        return lax.dot_general(
            q_ref[pl.ds(r, tile), :], k, (((1,), (1,)), ((), ())),
            preferred_element_type=jnp.float32,
        )

    if not first:
        acc[...] = acc_in[...]
        peak[...] = peak_in[...]
        total[...] = total_in[...]

    for (k_ref, v_ref), (flag, offset) in zip(pairs, offsets):

        def one(offset=offset, k_ref=k_ref, v_ref=v_ref):
            for r in range(0, rows, tile):
                here = pl.ds(r, tile)
                keys = r + tile if offset == 0 else rows
                s = scores_of(r, k_ref[pl.ds(0, keys), :])
                if offset == 0:
                    q_at = r + lax.broadcasted_iota(jnp.int32, s.shape, 0)
                    k_at = lax.broadcasted_iota(jnp.int32, s.shape, 1)
                    s = jnp.where((k_at <= q_at) & (k_at < facts[0]), s, -1e30)
                elif offset * rows + rows - 1 >= window:
                    q_at = r + lax.broadcasted_iota(jnp.int32, s.shape, 0)
                    k_at = lax.broadcasted_iota(jnp.int32, s.shape, 1)
                    s = jnp.where(offset * rows + q_at - k_at < window, s, -1e30)
                top = jnp.max(s, axis=1, keepdims=True)
                if offset == 0:
                    w = jnp.exp2((s - top) * scaling)
                    part = jnp.dot(
                        w.astype(jnp.bfloat16), v_ref[pl.ds(0, keys), :],
                        preferred_element_type=jnp.float32,
                    )
                    acc[here, :] = part
                    total[here, :] = jnp.broadcast_to(
                        jnp.sum(w, axis=1, keepdims=True), (tile, HEAD_DIM)
                    )
                    peak[here, :] = jnp.broadcast_to(top, (tile, HEAD_DIM))
                else:
                    old = peak[here, :]
                    new = jnp.maximum(old, top)
                    w = jnp.exp2((s - new[:, :1]) * scaling)
                    fade = jnp.exp2((old - new) * scaling)
                    part = jnp.dot(
                        w.astype(jnp.bfloat16), v_ref[...], preferred_element_type=jnp.float32
                    )
                    acc[here, :] = acc[here, :] * fade + part
                    total[here, :] = total[here, :] * fade + jnp.sum(w, axis=1, keepdims=True)
                    peak[here, :] = new

        if offset == 0:
            one()
        else:
            pl.when(facts[flag] > 0)(one)

    if last:
        out_ref[...] = (acc[...] / total[...]).astype(jnp.bfloat16)


def attend_stage(facts, queries, blocks, offsets, kv_heads, state, window, last):
    rows, width = queries.shape
    heads = width // HEAD_DIM
    group = heads // kv_heads
    tall = pl.BlockSpec((rows, HEAD_DIM), lambda h, f: (0, h))
    key_spec = pl.BlockSpec((rows, HEAD_DIM), lambda h, f: (0, h // group))
    value_spec = pl.BlockSpec((rows, HEAD_DIM), lambda h, f: (0, kv_heads + h // group))
    operands, specs = [queries], [tall]
    for block in blocks:
        operands += [block, block]
        specs += [key_spec, value_spec]
    if state is not None:
        operands += list(state)
        specs += [tall] * 3
    wide = jax.ShapeDtypeStruct((rows, width), jnp.float32)
    if last:
        out_shape = jax.ShapeDtypeStruct((rows, width), jnp.bfloat16)
        out_specs = tall
        scratch = [pltpu.VMEM((rows, HEAD_DIM), jnp.float32)] * 3
    else:
        out_shape, out_specs, scratch = (wide,) * 3, (tall,) * 3, []
    flops = 4 * rows * rows * width * len(offsets) * 3
    return pl.pallas_call(
        functools.partial(stage_kernel, offsets, window, state is None, last),
        out_shape=out_shape,
        grid_spec=pltpu.PrefetchScalarGridSpec(
            num_scalar_prefetch=1, grid=(heads,), in_specs=specs, out_specs=out_specs,
            scratch_shapes=scratch,
        ),
        compiler_params=pltpu.CompilerParams(
            dimension_semantics=("arbitrary",), vmem_limit_bytes=32 * 1024 * 1024
        ),
        cost_estimate=pl.CostEstimate(
            flops=flops, bytes_accessed=rows * width * 2 * (2 + 2 * len(offsets)),
            transcendentals=0,
        ),
    )(facts, *operands)


def shared_over_head(block):
    size = lax.axis_size("head")
    held = [block]
    step = size // 2
    got = {0: block}
    while step >= 1:
        for flip in sorted(got):
            got[flip ^ step] = None if got[flip] is None else swapped(got[flip], "head", step)
        step //= 2
    held = [got[flip] for flip in range(size)]
    return held


def sent(block, routes):
    return lax.ppermute(block, "seq", routes)


def row_gather(block):
    size = lax.axis_size("seq")
    me = lax.axis_index("seq")
    ring = [(i, (i + 2) % size) for i in range(size)]
    steps = []
    moving = block
    for step in range(size // 2):
        owner = lax.rem(me - 2 * step + size, size)
        across = swapped(moving, "seq", 1)
        onward = sent(moving, ring) if step + 1 < size // 2 else None
        moving, across, onward = yield moving, across, onward, owner
        moving = onward


def placed(whole, piece, owner):
    return lax.dynamic_update_slice_in_dim(whole, piece, owner * piece.shape[0], 0)


def waves(block, odd, beside):
    size = lax.axis_size("seq")
    first = sent(block, [(i, i + 1) for i in range(size - 1)])
    second_even = sent(block, [(i, i + 2) for i in range(0, size - 2, 2)])
    if beside is not None:
        first, beside = lax.optimization_barrier((first, beside))
    mixed = jnp.where(odd, block, first)
    second = sent(mixed, [(i, i + 2) for i in range(size - 2)])
    third_odd = sent(second_even, [(i, i + 1) for i in range(2, size, 2)])
    return first, [second_even, second, third_odd], beside


def local(
    residual, q_self, k_self, v_self, w_out, norm_gain, w_query, w_cache, block_doc, tail_len
):
    rows, width = q_self.shape
    local_heads = width // HEAD_DIM
    local_kv = w_cache.shape[1] // (2 * HEAD_DIM)
    seq_size, head_size = lax.axis_size("seq"), lax.axis_size("head")
    span = min(DOC_BLOCKS, seq_size // 2)
    far = list(range(1, span))
    me, my_head = lax.axis_index("seq"), lax.axis_index("head")

    own_doc = block_doc[me]
    following = jnp.where(me == seq_size - 1, -1, block_doc[jnp.minimum(me + 1, seq_size - 1)])
    live = jnp.where(following != own_doc, jnp.minimum(tail_len[me], rows), rows)
    odd = lax.rem(me, 2) == 1
    small = span == 4 and seq_size % 2 == 0

    def together(distance):
        other = me - distance
        return jnp.logical_and(other >= 0, block_doc[jnp.maximum(other, 0)] == own_doc)

    if small:
        flags = [
            together(1),
            jnp.logical_and(jnp.logical_not(odd), together(2)),
            jnp.where(odd, together(2), together(3)),
            jnp.logical_and(odd, together(3)),
        ]
        distances = [1, 2, 3, 3]
    else:
        flags = [together(distance) for distance in far]
        distances = far
    facts = jnp.stack([live.astype(jnp.int32)] + [flag.astype(jnp.int32) for flag in flags])
    slots = [(1 + i, distance) for i, distance in enumerate(distances)]

    stacked = jnp.concatenate([k_self, v_self], axis=1)
    weight_rows = jnp.concatenate([w_query, w_cache], axis=1)
    state = attend_stage(facts, q_self, [stacked], [(0, 0)], local_heads, None, WINDOW, False)
    if small:
        near, late, state = waves(stacked, odd, state)
    else:
        near, *late = [passed_along(stacked, "seq", offset) for offset in far]

    own_columns = residual.shape[1]
    out_pieces = []
    for flip in range(head_size):
        piece = lax.dynamic_slice_in_dim(w_out, (my_head ^ flip) * own_columns, own_columns, 1)
        out_pieces.append(piece if flip == 0 else swapped(piece, "head", flip))

    state = attend_stage(facts, q_self, [near], slots[:1], local_heads, state, WINDOW, False)
    if small:
        weight_rows, state = lax.optimization_barrier((weight_rows, state))
        weights = jnp.zeros((weight_rows.shape[0] * seq_size, weight_rows.shape[1]), jnp.bfloat16)
        gather = row_gather(weight_rows)
        moving, across, onward, owner = next(gather)
        late, across, onward, out_pieces = lax.optimization_barrier(
            (late, across, onward, out_pieces)
        )
        weights = placed(placed(weights, moving, owner), across, owner ^ 1)
        moving, across, onward, owner = gather.send((moving, across, onward))
    else:
        weights = lax.all_gather(weight_rows, "seq", axis=0, tiled=True)
    context = attend_stage(facts, q_self, late, slots[1:], local_heads, state, WINDOW, True)
    if small:
        context, across, onward = lax.optimization_barrier((context, across, onward))
        weights = placed(placed(weights, moving, owner), across, owner ^ 1)
        moving, across, onward, owner = gather.send((moving, across, onward))

    contexts = shared_over_head(context)
    projected = jnp.dot(contexts[0], out_pieces[0], preferred_element_type=jnp.float32)
    for flip in range(1, head_size):
        projected += jnp.dot(contexts[flip], out_pieces[flip], preferred_element_type=jnp.float32)
    hidden = (residual.astype(jnp.float32) + projected).astype(jnp.bfloat16)
    if small:
        hidden, across, onward = lax.optimization_barrier((hidden, across, onward))
        weights = placed(placed(weights, moving, owner), across, owner ^ 1)
        while onward is not None:
            moving, across, onward, owner = gather.send((moving, across, onward))
            weights = placed(placed(weights, moving, owner), across, owner ^ 1)

    full = jnp.zeros((rows, own_columns * head_size), jnp.bfloat16)
    for flip, piece in enumerate(shared_over_head(hidden)):
        full = lax.dynamic_update_slice_in_dim(full, piece, (my_head ^ flip) * own_columns, 1)
    wide = full.astype(jnp.float32)
    mean_square = jnp.sum(wide * wide, axis=1, keepdims=True) / D
    normed = (wide * lax.rsqrt(mean_square + EPSILON) * norm_gain).astype(jnp.bfloat16)

    cache_rows = jnp.dot(
        normed, weights[:, width:], preferred_element_type=jnp.float32
    ).astype(jnp.bfloat16)
    if small:
        near, late, _ = waves(cache_rows, odd, None)
    else:
        near, *late = [passed_along(cache_rows, "seq", offset) for offset in far]
    cross_queries = jnp.dot(
        normed, weights[:, :width], preferred_element_type=jnp.float32
    ).astype(jnp.bfloat16)
    reach = DOC_BLOCKS * rows
    state = attend_stage(
        facts, cross_queries, [cache_rows, near], [(0, 0)] + slots[:1], local_kv, None, reach, False
    )
    cross_context = attend_stage(
        facts, cross_queries, late, slots[1:], local_kv, state, reach, True
    )
    return (hidden, cross_context)


def solution(mesh):
    in_specs = (
        P("seq", "head"),
        P("seq", "head"),
        P("seq", "head"),
        P("seq", "head"),
        P("head", None),
        P(),
        P("seq", "head"),
        P("seq", "head"),
        P(),
        P(),
    )
    out_specs = (P("seq", "head"), P("seq", "head"))
    return jax.shard_map(local, mesh=mesh, in_specs=in_specs, out_specs=out_specs, check_vma=False)
```
